32 devices in a mesh: lat: 4 (over y, x), lon: 8 (over z, core).
Axes of the slice: x: 2, y: 2, z: 4, core: 2. Of those that a mesh axis runs over, the one named last changes fastest.
Arguments:
- right_side: float32 [8, 768, 1024], P(None, 'lat', 'lon'), may hold values from -16 to 16
- center: float32 [768, 1024], P('lat', 'lon'), may hold values from 3.7 to 5.5
- couplings: float32 [4, 768, 1024], P(None, 'lat', 'lon'), may hold values from 0.15 to 0.45
- land_sea: int32 [768, 1024], P('lat', 'lon'), may hold values 0 or 1
- fold_partner: int32 [1024], replicated, may hold values from 0 to 1023, as said below
Outputs:
- solution: float32 [8, 768, 1024], P(None, 'lat', 'lon')
- residual: float32 [8, 768, 1024], P(None, 'lat', 'lon')
The draws below stay inside these ranges and needn't reach their ends.
Inputs may be any that keep to these rules, and one draw needn't show every extreme that they name: fold_partner[i] = (s - i) mod 1024 for one integer s, so fold_partner[fold_partner[i]] = i.
All inputs are finite; a program needn't handle non-finite values. No bound on the sum of `land_sea` on one device may be relied on, other than what follows from the above.
Results may differ from the reference program's by a relative error of at most 0.0003.
Values sent between devices are 32-bit elements; how exact they have to be, the bound alone decides.
A program may use at most 64 MiB of HBM per device.

```python
import math
import jax
import jax.numpy as jnp
from jax import lax

MEMBERS = 8
ITERS = 3
NLAT = 768
NLON = 1024


def draw_right_side(key, part):
    first_key = jax.random.fold_in(key, 11)
    row_pos = jnp.arange(NLAT, dtype=jnp.float32) / NLAT
    col_pos = jnp.arange(NLON, dtype=jnp.float32) / NLON
    scale_map = jnp.exp(0.55 * (row_pos[:, None] + col_pos[None, :]))
    base = jnp.clip(jax.random.normal(first_key, (MEMBERS, NLAT, NLON), jnp.float32), -4.0, 4.0)
    values = base * scale_map[None]
    return values.astype(jnp.float32)


def draw_fold_partner(key, part):
    offset = jax.random.randint(jax.random.fold_in(key, 21), (), 0, NLON)
    return ((offset - jnp.arange(NLON, dtype=jnp.int32)) % NLON).astype(jnp.int32)


def touch_ends(values, rng, least, top_value):
    longest = values.shape.index(max(values.shape))
    spots = []
    for shift in (0, 1):
        where = [jax.random.randint(jax.random.fold_in(rng, axis), (), 0, length) for axis, length in enumerate(values.shape)]
        where[longest] = (where[longest] + shift) % values.shape[longest]
        spots.append(tuple(where))
    return values.at[spots[0]].set(least).at[spots[1]].set(top_value)


def block_scale(key, shape, shards, low, top_value):
    def one(axis_at, blocks):
        steps = jax.random.uniform(jax.random.fold_in(jax.random.fold_in(key, 6), axis_at), (blocks,), jnp.float32, low / len(shards), top_value / len(shards))
        return jnp.repeat(jnp.exp(steps), shape[axis_at] // blocks).reshape((-1,) + (1,) * (len(shape) - axis_at - 1))

    loudness = one(*shards[0])
    for cut in shards[1:]:
        loudness = loudness * one(*cut)
    return loudness


def setup_inputs(seed: int = 0) -> dict:
    arg_keys = jax.random.split(jax.random.key(seed), 6)
    return {
        "right_side": draw_right_side(jax.random.fold_in(arg_keys[5], 71), 0),
        "center": jnp.clip(3.7 + 1.8 * jax.random.uniform(arg_keys[1], (NLAT, NLON), jnp.float32) ** block_scale(arg_keys[1], (NLAT, NLON), ((0, 4), (1, 8)), -0.2, 0.2), 3.7, 5.5),
        "couplings": jnp.clip(jnp.exp(math.log(0.45) - 1.0986122 * jax.random.uniform(arg_keys[2], (4, NLAT, NLON), jnp.float32) ** block_scale(arg_keys[2], (4, NLAT, NLON), ((1, 4), (2, 8)), -0.2, 0.2)), 0.15, 0.45),
        "land_sea": touch_ends((jax.random.randint(arg_keys[3], (NLAT, NLON), 0, 5) < 4).astype(jnp.int32), jax.random.fold_in(arg_keys[3], 1), 0, 1),
        "fold_partner": draw_fold_partner(jax.random.fold_in(arg_keys[5], 71), 0),
    }


def below(values):
    return jnp.concatenate([jnp.zeros_like(values[:1]), values[:-1]], axis=0)


def reference(right_side, center, couplings, land_sea, fold_partner):
    ocean_mask = land_sea.astype(jnp.float32)
    east_coeff = couplings[0]
    north_top = couplings[1][-1]
    fold_coeff = 0.5 * (north_top + north_top[fold_partner])
    top_rows = (jnp.arange(NLAT) == NLAT - 1)[:, None]
    north_coeff = jnp.where(top_rows, fold_coeff[None, :], couplings[1])
    northeast = jnp.where(top_rows, 0.0, couplings[2])
    northwest = jnp.where(top_rows, 0.0, couplings[3])
    west_coeff = jnp.roll(east_coeff, 1, axis=1)
    south_coeff = below(north_coeff)
    southwest = jnp.roll(below(northeast), 1, axis=1)
    southeast = jnp.roll(below(northwest), -1, axis=1)

    def operate(vector):
        fold_ghost = vector[-1][fold_partner]
        upper = jnp.concatenate([vector[1:], fold_ghost[None, :]], axis=0)
        lower = below(vector)
        beside = east_coeff * jnp.roll(vector, -1, axis=1) + west_coeff * jnp.roll(vector, 1, axis=1)
        beside = beside + north_coeff * upper + south_coeff * lower
        beside = beside + northeast * jnp.roll(upper, -1, axis=1) + southwest * jnp.roll(lower, 1, axis=1)
        beside = beside + northwest * jnp.roll(upper, 1, axis=1) + southeast * jnp.roll(lower, -1, axis=1)
        return ocean_mask * (center * vector - beside)

    def solve_one(member_rhs):
        residual = ocean_mask * member_rhs
        solution = jnp.zeros_like(residual)
        scaled = residual / center
        direction = scaled
        gamma_now = jnp.sum(residual * scaled)
        for iteration in range(ITERS):
            image = operate(direction)
            step_size = gamma_now / jnp.sum(direction * image)
            solution = solution + step_size * direction
            residual = residual - step_size * image
            scaled = residual / center
            gamma_next = jnp.sum(residual * scaled)
            direction = scaled + (gamma_next / gamma_now) * direction
            gamma_now = gamma_next
        return solution, residual

    solution, residual = lax.map(solve_one, right_side)
    return solution, residual
```

```python
import functools

import jax
import jax.numpy as jnp
from jax import lax
from jax.experimental import pallas as pl
from jax.experimental.pallas import tpu as pltpu
from jax.sharding import PartitionSpec as P

ITERS = 3
MESH = pl.DeviceIdType.MESH
S_, SE_, SW_, N_, NE_, NW_ = range(6)


def kernel(
    lat_count, lon_count,
    rhs, center_hbm, coup_hbm, land_hbm, partner_hbm, sol_out, res_out,
    w, obuf, center, coup, land, partner,
    dmask, coef, rowtop, rowbot, colw, cole, rrow, rcol, rfold, red, rred_lon, rred_lat,
    load_sem, store_sem, row_ss, row_rs, col_ss, col_rs, fold_ss, fold_rs,
    rl_ss, rl_rs, rt_ss, rt_rs,
):
    f32 = jnp.float32
    members, rows, cols = rhs.shape
    groups = rows // 8
    halves = -(-rows // 120)
    half = rows // halves
    hgroups = half // 8
    la, lo = lax.axis_index("lat"), lax.axis_index("lon")
    lat_first, lat_last = la == 0, la == lat_count - 1
    north, south = lax.rem(la + 1, lat_count), lax.rem(la + lat_count - 1, lat_count)
    east, west = lax.rem(lo + 1, lon_count), lax.rem(lo + lon_count - 1, lon_count)
    lane = lax.broadcasted_iota(jnp.int32, (members, cols), 1)
    sub = lax.broadcasted_iota(jnp.int32, (8, cols), 0)

    loads = [
        pltpu.make_async_copy(center_hbm, center, load_sem.at[0]),
        pltpu.make_async_copy(coup_hbm, coup, load_sem.at[1]),
        pltpu.make_async_copy(land_hbm, land, load_sem.at[2]),
        pltpu.make_async_copy(partner_hbm, partner, load_sem.at[3]),
    ]
    for m in range(members):
        loads.append(pltpu.make_async_copy(
            rhs.at[m], w.at[0, pl.ds(0, rows), m], load_sem.at[4 + m]))
    for c in loads:
        c.start()

    barrier = pltpu.get_barrier_semaphore()
    partners = [(la, lax.rem(lo + d, lon_count)) for d in range(1, lon_count)]
    partners += [(lax.rem(la + d, lat_count), lo) for d in range(1, lat_count)]
    partners += [(north, east), (north, west), (south, east), (south, west)]
    for p in partners:
        pl.semaphore_signal(barrier, inc=1, device_id=p, device_id_type=MESH)

    for c in loads:
        c.wait()

    def roll(x, shift, axis=1):
        return pltpu.roll(x, shift, axis)

    for h in range(halves):
        def prep(gl, carry):
            pw, pe = carry
            g = h * hgroups + gl
            rs = pl.ds(pl.multiple_of(g * 8, 8), 8)
            dmask[rs, :] = land[rs, :].astype(f32) / center[rs, :]
            for r in range(8):
                j = g * 8 + r
                v = w[0, j] * dmask[pl.ds(j, 1), :]
                w[0, j] = v
                here = lane == gl * 8 + r
                pw = jnp.where(here, v[:, 0:1], pw)
                pe = jnp.where(here, v[:, cols - 1:cols], pe)
            return pw, pe
        zero = jnp.zeros((members, cols), f32)
        pw, pe = lax.fori_loop(0, hgroups, prep, (zero, zero))
        colw[0, h] = pw
        cole[0, h] = pe
    cw = jnp.zeros((8, cols), f32)
    ce = jnp.zeros((8, cols), f32)
    for g in range(groups):
        rs = pl.ds(g * 8, 8)
        ce = jnp.where(lane == g, coup[0, rs, cols - 1:cols], ce)
        ce = jnp.where(lane == groups + g, coup[2, rs, cols - 1:cols], ce)
        cw = jnp.where(lane == g, coup[3, rs, 0:1], cw)
    colw[0, halves] = cw
    cole[0, halves] = ce
    rowtop[0, 0] = w[0, rows - 1]
    rowbot[0, 0] = w[0, 0]
    top = [coup[c, pl.ds(rows - 1, 1), :] for c in range(4)]
    packed = jnp.zeros((8, cols), f32)
    for c in (1, 2, 3):
        packed = jnp.where(sub == c, top[c], packed)
    rowtop[0, 1] = packed

    pl.semaphore_wait(barrier, len(partners))

    def exchange(k):
        tops = 2 if k == 0 else 1
        depth = halves + 1 if k == 0 else halves
        cps = []

        def rcopy(src, slot, n, dev):
            cps.append(pltpu.make_async_remote_copy(
                src_ref=src.at[k, pl.ds(0, n)], dst_ref=rrow.at[k, slot, pl.ds(0, n)],
                send_sem=row_ss.at[k, slot], recv_sem=row_rs.at[k, slot],
                device_id=dev, device_id_type=MESH))
        rcopy(rowtop, SW_, tops, (north, east))
        rcopy(rowtop, SE_, tops, (north, west))
        rcopy(rowbot, NW_, 1, (south, east))
        rcopy(rowbot, NE_, 1, (south, west))
        rcopy(rowtop, S_, tops, (north, lo))
        rcopy(rowbot, N_, 1, (south, lo))
        for src, side, dev in ((colw, 0, west), (cole, 1, east)):
            cps.append(pltpu.make_async_remote_copy(
                src_ref=src.at[k, pl.ds(0, depth)], dst_ref=rcol.at[k, side, pl.ds(0, depth)],
                send_sem=col_ss.at[k, side], recv_sem=col_rs.at[k, side],
                device_id=(la, dev), device_id_type=MESH))
        folds = []
        for d in range(1, lon_count):
            folds.append(pltpu.make_async_remote_copy(
                src_ref=rowtop.at[k, pl.ds(0, tops)], dst_ref=rfold.at[k, d, pl.ds(0, tops)],
                send_sem=fold_ss.at[k, d], recv_sem=fold_rs.at[k, d],
                device_id=(la, lax.rem(lo + d, lon_count)), device_id_type=MESH))

        @pl.when(lat_last)
        def _():
            for c in folds:
                c.start()
        for c in cps:
            c.start()
        for c in cps:
            c.wait_recv()

        @pl.when(lat_last)
        def _():
            for c in folds:
                c.wait_recv()
        return cps, folds

    def folded(k, slot, own):
        mine = partner[pl.ds(lo, 1), :]
        out = jnp.zeros((8, cols), f32)
        for d in range(lon_count):
            data = own if d == 0 else rfold[k, d, slot]
            first = lax.rem(lo + lon_count - d, lon_count) * cols
            at = jnp.broadcast_to(mine - first, (8, cols))
            inside = jnp.logical_and(at >= 0, at < cols)
            at = jnp.clip(at, 0, cols - 1)
            got = jnp.take_along_axis(data, at, axis=1, mode="promise_in_bounds")
            out = jnp.where(inside, got, out)
        return out

    done = []
    lane8 = lax.broadcasted_iota(jnp.int32, (8, cols), 1)

    def coefficients():
        smsg, semsg, swmsg = rrow[0, S_, 1], rrow[0, SE_, 1], rrow[0, SW_, 1]
        keep = jnp.where(lat_first, 0.0, 1.0).astype(f32)
        under_n = roll(smsg, 7, 0) * keep
        under_ne = roll(roll(jnp.where(lane8 == cols - 1, swmsg, smsg), 1), 6, 0) * keep
        under_nw = roll(roll(jnp.where(lane8 == 0, semsg, smsg), cols - 1), 5, 0) * keep
        from_east, from_west = rcol[0, 0, halves], rcol[0, 1, halves]

        @pl.when(lat_last)
        def _():
            got = folded(0, 1, rowtop[0, 1])
            last = rows - 1
            coup[1, pl.ds(last, 1), :] = 0.5 * (coup[1, pl.ds(last, 1), :] + got[1:2, :])
            coup[2, pl.ds(last, 1), :] = jnp.zeros((1, cols), f32)
            coup[3, pl.ds(last, 1), :] = jnp.zeros((1, cols), f32)

        def step(g, carry):
            pn, pne, pnw = carry
            rs = pl.ds(pl.multiple_of(g * 8, 8), 8)
            d = dmask[rs, :]
            e, n, ne, nw = (coup[c, rs, :] for c in range(4))
            gw = roll(from_west, lax.rem(2 * cols - 1 - g, cols))
            gne = roll(from_west, lax.rem(2 * cols - 1 - groups - g, cols))
            gnw = roll(from_east, lax.rem(cols - g, cols))
            coef[0, rs, :] = e * d
            coef[1, rs, :] = roll(jnp.where(lane8 == cols - 1, gw, e), 1) * d
            coef[2, rs, :] = n * d
            ns = roll(n, 1, 0)
            coef[3, rs, :] = jnp.where(sub == 0, pn, ns) * d
            coef[4, rs, :] = ne * d
            nes = roll(roll(jnp.where(lane8 == cols - 1, gne, ne), 1), 1, 0)
            coef[5, rs, :] = jnp.where(sub == 0, pne, nes) * d
            coef[6, rs, :] = nw * d
            nws = roll(roll(jnp.where(lane8 == 0, gnw, nw), cols - 1), 1, 0)
            coef[7, rs, :] = jnp.where(sub == 0, pnw, nws) * d
            return ns, nes, nws
        lax.fori_loop(0, groups, step, (under_n, under_ne, under_nw))

    zero = jnp.zeros((members, cols), f32)
    moments = jnp.zeros((members, cols), f32)
    for k in range(ITERS):
        done.append(exchange(k))
        if k == 0:
            coefficients()
        w[k, rows] = rrow[k, N_, 0]

        @pl.when(lat_last)
        def _():
            w[k, rows] = folded(k, 0, w[k, rows - 1])

        def sides(v, ge, gw):
            ve = roll(jnp.where(lane == 0, ge, v), cols - 1)
            vw = roll(jnp.where(lane == cols - 1, gw, v), 1)
            return v, ve, vw

        prev = sides(rrow[k, S_, 0], rrow[k, SE_, 0], rrow[k, SW_, 0])
        gws, ges = [], []
        for h in range(halves):
            if h + 1 < halves:
                fe = roll(rcol[k, 0, h + 1], half)
                fw = roll(rcol[k, 1, h + 1], half)
            else:
                fe = roll(rrow[k, NE_, 0], half)
                fw = roll(rrow[k, NW_, 0], half + 1)
            ges.append(jnp.where(lane == half, fe, rcol[k, 0, h]))
            gws.append(jnp.where(lane == half, fw, rcol[k, 1, h]))
        cur = sides(w[k, 0], ges[0], roll(gws[0], cols - 1))
        acc0, acc1 = zero, zero
        for h in range(halves):
            ge_h, gw_h = ges[h], gws[h]

            def step(gl, carry):
                prev, cur, acc0, acc1, pw, pe = carry
                g = h * hgroups + gl
                back = lax.rem(cols - gl * 8, cols)
                ge = roll(ge_h, back)
                gw = roll(gw_h, back)
                for r in range(8):
                    j = g * 8 + r
                    nxt = sides(w[k, j + 1], roll(ge, cols - 1 - r), roll(gw, cols - 2 - r))
                    c = [coef[q, pl.ds(j, 1), :] for q in range(8)]
                    out = (c[0] * cur[1] + c[1] * cur[2]) + (c[2] * nxt[0] + c[3] * prev[0])
                    out = out + ((c[4] * nxt[1] + c[5] * prev[2]) + (c[6] * nxt[2] + c[7] * prev[1]))
                    w[k + 1, j] = out
                    t = center[pl.ds(j, 1), :] * cur[0]
                    acc0 = acc0 + t * cur[0]
                    acc1 = acc1 + t * out
                    if k + 1 < ITERS:
                        here = lane == gl * 8 + r
                        pw = jnp.where(here, out[:, 0:1], pw)
                        pe = jnp.where(here, out[:, cols - 1:cols], pe)
                    prev, cur = cur, nxt
                return prev, cur, acc0, acc1, pw, pe
            prev, cur, acc0, acc1, pw, pe = lax.fori_loop(
                0, hgroups, step, (prev, cur, acc0, acc1, zero, zero))
            if k + 1 < ITERS:
                colw[k + 1, h] = pw
                cole[k + 1, h] = pe
        if k + 1 < ITERS:
            rowtop[k + 1, 0] = w[k + 1, rows - 1]
            rowbot[k + 1, 0] = w[k + 1, 0]
        moments = jnp.where(lane == 2 * k, jnp.sum(acc0, axis=1, keepdims=True), moments)
        moments = jnp.where(lane == 2 * k + 1, jnp.sum(acc1, axis=1, keepdims=True), moments)

    def reduce(slot, value, recv, ss, rs, count, dev):
        red[slot] = value
        cps = [
            pltpu.make_async_remote_copy(
                src_ref=red.at[slot], dst_ref=recv.at[d], send_sem=ss.at[d],
                recv_sem=rs.at[d], device_id=dev(d), device_id_type=MESH)
            for d in range(1, count)
        ]
        for c in cps:
            c.start()
        for c in cps:
            c.wait_recv()
        for d in range(1, count):
            value = value + recv[d]
        return value, cps

    moments, c1 = reduce(0, moments, rred_lon, rl_ss, rl_rs, lon_count,
                         lambda d: (la, lax.rem(lo + d, lon_count)))
    moments, c2 = reduce(1, moments, rred_lat, rt_ss, rt_rs, lat_count,
                         lambda d: (lax.rem(la + d, lat_count), lo))

    m0, m1, m2, m3, m4, m5 = (
        jnp.broadcast_to(moments[:, i:i + 1], (members, cols)) for i in range(6))
    a0 = m1 / m0
    h1 = m2 - a0 * m1
    a1 = (m3 - 2.0 * a0 * m2 + a0 * a0 * m1) / h1
    b1 = h1 / m0
    p1 = -(a0 + a1)
    p0 = a0 * a1 - b1
    h2 = m4 + p1 * m3 + p0 * m2
    a2 = (m5 + p1 * m4 + p0 * m3) / h2 + p1
    b2 = h2 / h1
    t2 = p1 - a2
    t1 = p0 - a2 * p1 - b2
    t0 = b2 * a0 - a2 * p0
    q3 = 1.0 / (1.0 + t2 + t1 + t0)
    q2, q1, q0 = t2 * q3, t1 * q3, t0 * q3
    s2, s1, s0 = q3, q2 + q3, q1 + q2 + q3

    chunk = 4
    stores = []
    for c in range(chunk):
        size = groups // chunk

        def final(g, carry):
            for r in range(8):
                j = (c * size + g) * 8 + r
                v0, v1, v2, v3 = (w[i, j] for i in range(4))
                obuf[0, j] = s0 * v0 + s1 * v1 + s2 * v2
                obuf[1, j] = center[pl.ds(j, 1), :] * (q0 * v0 + q1 * v1 + q2 * v2 + q3 * v3)
            return carry
        lax.fori_loop(0, size, final, 0)
        rs = pl.ds(c * size * 8, size * 8)
        for o, dst in ((0, sol_out), (1, res_out)):
            for m in range(members):
                cp = pltpu.make_async_copy(
                    obuf.at[o, rs, m], dst.at[m, rs], store_sem.at[c, o, m])
                cp.start()
                stores.append(cp)
    for cps, folds in done:
        for cp in cps:
            cp.wait_send()

        @pl.when(lat_last)
        def _():
            for cp in folds:
                cp.wait_send()
    for cp in c1 + c2:
        cp.wait_send()
    for cp in stores:
        cp.wait()


def body(lat_count, lon_count, right_side, center, couplings, land_sea, fold_partner):
    members, rows, cols = right_side.shape
    f32 = jnp.float32
    halves = -(-rows // 120)
    hbm = pl.BlockSpec(memory_space=pl.ANY)
    dma = pltpu.SemaphoreType.DMA
    shape = jax.ShapeDtypeStruct(right_side.shape, f32)
    return pl.pallas_call(
        functools.partial(kernel, lat_count, lon_count),
        out_shape=(shape, shape),
        in_specs=[hbm] * 5,
        out_specs=(hbm, hbm),
        scratch_shapes=[
            pltpu.VMEM((ITERS + 1, rows + 1, members, cols), f32),
            pltpu.VMEM((2, rows, members, cols), f32),
            pltpu.VMEM((rows, cols), f32),
            pltpu.VMEM((4, rows, cols), f32),
            pltpu.VMEM((rows, cols), jnp.int32),
            pltpu.VMEM((lon_count, cols), jnp.int32),
            pltpu.VMEM((rows, cols), f32),
            pltpu.VMEM((8, rows, cols), f32),
            pltpu.VMEM((ITERS, 2, 8, cols), f32),
            pltpu.VMEM((ITERS, 1, 8, cols), f32),
            pltpu.VMEM((ITERS, halves + 1, 8, cols), f32),
            pltpu.VMEM((ITERS, halves + 1, 8, cols), f32),
            pltpu.VMEM((ITERS, 6, 2, 8, cols), f32),
            pltpu.VMEM((ITERS, 2, halves + 1, 8, cols), f32),
            pltpu.VMEM((ITERS, lon_count, 2, 8, cols), f32),
            pltpu.VMEM((2, 8, cols), f32),
            pltpu.VMEM((lon_count, 8, cols), f32),
            pltpu.VMEM((lat_count, 8, cols), f32),
            dma((4 + members,)),
            dma((4, 2, members)),
            dma((ITERS, 6)), dma((ITERS, 6)),
            dma((ITERS, 2)), dma((ITERS, 2)),
            dma((ITERS, lon_count)), dma((ITERS, lon_count)),
            dma((lon_count,)), dma((lon_count,)),
            dma((lat_count,)), dma((lat_count,)),
        ],
        compiler_params=pltpu.CompilerParams(
            collective_id=0, has_side_effects=True, vmem_limit_bytes=40 * 1024 * 1024),
    )(right_side, center, couplings, land_sea, fold_partner.reshape(lon_count, cols))


def solution(mesh):
    return jax.shard_map(
        functools.partial(body, mesh.shape["lat"], mesh.shape["lon"]),
        mesh=mesh,
        in_specs=(
            P(None, "lat", "lon"),
            P("lat", "lon"),
            P(None, "lat", "lon"),
            P("lat", "lon"),
            P(),
        ),
        out_specs=(P(None, "lat", "lon"), P(None, "lat", "lon")),
        check_vma=False,
    )
```

```python
import functools

import jax
import jax.numpy as jnp
from jax import lax
from jax.experimental import pallas as pl
from jax.experimental.pallas import tpu as pltpu
from jax.sharding import PartitionSpec as P

ITERS = 3
MESH = pl.DeviceIdType.MESH
S_, SE_, SW_, N_, NE_, NW_ = range(6)


def kernel(
    lat_count, lon_count,
    rhs, center_hbm, coup_hbm, land_hbm, partner_hbm, sol_out, res_out,
    w, obuf, center, coup, land, partner,
    dmask, coef, rowtop, rowbot, colw, cole, rrow, rcol, rfold, red, rred_lon, rred_lat,
    load_sem, store_sem, row_ss, row_rs, col_ss, col_rs, fold_ss, fold_rs,
    rl_ss, rl_rs, rt_ss, rt_rs,
):
    f32 = jnp.float32
    members, rows, cols = rhs.shape
    groups = rows // 8
    halves = -(-rows // 120)
    half = rows // halves
    step_rows = 16 if half % 16 == 0 else 8
    steps = half // step_rows
    la, lo = lax.axis_index("lat"), lax.axis_index("lon")
    lat_first, lat_last = la == 0, la == lat_count - 1
    north, south = lax.rem(la + 1, lat_count), lax.rem(la + lat_count - 1, lat_count)
    east, west = lax.rem(lo + 1, lon_count), lax.rem(lo + lon_count - 1, lon_count)
    lane = lax.broadcasted_iota(jnp.int32, (members, cols), 1)
    sub = lax.broadcasted_iota(jnp.int32, (8, cols), 0)

    loads = [
        pltpu.make_async_copy(center_hbm, center, load_sem.at[0]),
        pltpu.make_async_copy(coup_hbm, coup, load_sem.at[1]),
        pltpu.make_async_copy(land_hbm, land, load_sem.at[2]),
        pltpu.make_async_copy(partner_hbm, partner, load_sem.at[3]),
    ]
    for m in range(members):
        loads.append(pltpu.make_async_copy(
            rhs.at[m], w.at[0, pl.ds(0, rows), m], load_sem.at[4 + m]))
    for c in loads:
        c.start()

    barrier = pltpu.get_barrier_semaphore()
    partners = [(la, lax.rem(lo + d, lon_count)) for d in range(1, lon_count)]
    partners += [(lax.rem(la + d, lat_count), lo) for d in range(1, lat_count)]
    partners += [(north, east), (north, west), (south, east), (south, west)]
    for p in partners:
        pl.semaphore_signal(barrier, inc=1, device_id=p, device_id_type=MESH)

    for c in loads:
        c.wait()

    def roll(x, shift, axis=1):
        return pltpu.roll(x, shift, axis)

    def packed_step(pw, pe, values):
        pw, pe = roll(pw, cols - step_rows), roll(pe, cols - step_rows)
        for r, v in enumerate(values):
            at = cols - step_rows + r
            pw = jnp.where(lane == at, roll(v, at), pw)
            pe = jnp.where(lane == at, roll(v, (at + 1) % cols), pe)
        return pw, pe

    for h in range(halves):
        def prep(gl, carry):
            pw, pe = carry
            j0 = pl.multiple_of((h * steps + gl) * step_rows, 8)
            rs = pl.ds(j0, step_rows)
            dmask[rs, :] = land[rs, :].astype(f32) / center[rs, :]
            values = []
            for r in range(step_rows):
                v = w[0, j0 + r] * dmask[pl.ds(j0 + r, 1), :]
                w[0, j0 + r] = v
                values.append(v)
            return packed_step(pw, pe, values)
        zero = jnp.zeros((members, cols), f32)
        pw, pe = lax.fori_loop(0, steps, prep, (zero, zero))
        colw[0, h] = roll(pw, half)
        cole[0, h] = roll(pe, half)
    cw = jnp.zeros((8, cols), f32)
    ce = jnp.zeros((8, cols), f32)
    for g in range(groups):
        rs = pl.ds(g * 8, 8)
        ce = jnp.where(lane == g, roll(coup[0, rs, :], g + 1), ce)
        ce = jnp.where(lane == groups + g, roll(coup[2, rs, :], groups + g + 1), ce)
        cw = jnp.where(lane == g, roll(coup[3, rs, :], g) if g else coup[3, rs, :], cw)
    colw[0, halves] = cw
    cole[0, halves] = ce
    rowtop[0, 0] = w[0, rows - 1]
    rowbot[0, 0] = w[0, 0]
    top = [coup[c, pl.ds(rows - 1, 1), :] for c in range(4)]
    packed = jnp.zeros((8, cols), f32)
    for c in (1, 2, 3):
        packed = jnp.where(sub == c, top[c], packed)
    rowtop[0, 1] = packed

    pl.semaphore_wait(barrier, len(partners))

    def exchange(k, between):
        tops = 2 if k == 0 else 1
        depth = halves + 1 if k == 0 else halves
        cps = []

        def rcopy(src, slot, n, dev):
            cps.append(pltpu.make_async_remote_copy(
                src_ref=src.at[k, pl.ds(0, n)], dst_ref=rrow.at[k, slot, pl.ds(0, n)],
                send_sem=row_ss.at[k, slot], recv_sem=row_rs.at[k, slot],
                device_id=dev, device_id_type=MESH))
        rcopy(rowtop, SW_, tops, (north, east))
        rcopy(rowtop, SE_, tops, (north, west))
        rcopy(rowbot, NW_, 1, (south, east))
        rcopy(rowbot, NE_, 1, (south, west))
        rcopy(rowtop, S_, tops, (north, lo))
        rcopy(rowbot, N_, 1, (south, lo))
        for src, side, dev in ((colw, 0, west), (cole, 1, east)):
            cps.append(pltpu.make_async_remote_copy(
                src_ref=src.at[k, pl.ds(0, depth)], dst_ref=rcol.at[k, side, pl.ds(0, depth)],
                send_sem=col_ss.at[k, side], recv_sem=col_rs.at[k, side],
                device_id=(la, dev), device_id_type=MESH))
        folds = []
        for d in range(1, lon_count):
            folds.append(pltpu.make_async_remote_copy(
                src_ref=rowtop.at[k, pl.ds(0, tops)], dst_ref=rfold.at[k, d, pl.ds(0, tops)],
                send_sem=fold_ss.at[k, d], recv_sem=fold_rs.at[k, d],
                device_id=(la, lax.rem(lo + d, lon_count)), device_id_type=MESH))

        @pl.when(lat_last)
        def _():
            for c in folds:
                c.start()
        for c in cps:
            c.start()
        between()
        for c in cps:
            c.wait_recv()

        @pl.when(lat_last)
        def _():
            for c in folds:
                c.wait_recv()
        return cps, folds

    def folded(k, slot, own):
        mine = partner[pl.ds(lo, 1), :]
        out = jnp.zeros((8, cols), f32)
        for d in range(lon_count):
            data = own if d == 0 else rfold[k, d, slot]
            first = lax.rem(lo + lon_count - d, lon_count) * cols
            at = jnp.broadcast_to(mine - first, (8, cols))
            inside = jnp.logical_and(at >= 0, at < cols)
            at = jnp.clip(at, 0, cols - 1)
            got = jnp.take_along_axis(data, at, axis=1, mode="promise_in_bounds")
            out = jnp.where(inside, got, out)
        return out

    done = []
    lane8 = lax.broadcasted_iota(jnp.int32, (8, cols), 1)

    def coefficients():
        smsg, semsg, swmsg = rrow[0, S_, 1], rrow[0, SE_, 1], rrow[0, SW_, 1]
        keep = jnp.where(lat_first, 0.0, 1.0).astype(f32)
        under_n = roll(smsg, 7, 0) * keep
        under_ne = roll(roll(jnp.where(lane8 == cols - 1, swmsg, smsg), 1), 6, 0) * keep
        under_nw = roll(roll(jnp.where(lane8 == 0, semsg, smsg), cols - 1), 5, 0) * keep
        from_east, from_west = rcol[0, 0, halves], rcol[0, 1, halves]

        @pl.when(lat_last)
        def _():
            got = folded(0, 1, rowtop[0, 1])
            last = rows - 1
            coup[1, pl.ds(last, 1), :] = 0.5 * (coup[1, pl.ds(last, 1), :] + got[1:2, :])
            coup[2, pl.ds(last, 1), :] = jnp.zeros((1, cols), f32)
            coup[3, pl.ds(last, 1), :] = jnp.zeros((1, cols), f32)

        def step(g, carry):
            pn, pne, pnw = carry
            rs = pl.ds(pl.multiple_of(g * 8, 8), 8)
            d = dmask[rs, :]
            e, n, ne, nw = (coup[c, rs, :] for c in range(4))
            gw = roll(from_west, lax.rem(2 * cols - 1 - g, cols))
            gne = roll(from_west, lax.rem(2 * cols - 1 - groups - g, cols))
            gnw = roll(from_east, lax.rem(cols - g, cols))
            coef[0, rs, :] = e * d
            coef[1, rs, :] = roll(jnp.where(lane8 == cols - 1, gw, e), 1) * d
            coef[2, rs, :] = n * d
            ns = roll(n, 1, 0)
            coef[3, rs, :] = jnp.where(sub == 0, pn, ns) * d
            coef[4, rs, :] = ne * d
            nes = roll(roll(jnp.where(lane8 == cols - 1, gne, ne), 1), 1, 0)
            coef[5, rs, :] = jnp.where(sub == 0, pne, nes) * d
            coef[6, rs, :] = nw * d
            nws = roll(roll(jnp.where(lane8 == 0, gnw, nw), cols - 1), 1, 0)
            coef[7, rs, :] = jnp.where(sub == 0, pnw, nws) * d
            return ns, nes, nws
        lax.fori_loop(0, groups, step, (under_n, under_ne, under_nw))

    zero = jnp.zeros((members, cols), f32)
    sums = []

    def add_sums():
        for acc in accs:
            sums.append(jnp.sum(acc, axis=1, keepdims=True))

    accs = []
    for k in range(ITERS):
        done.append(exchange(k, add_sums))
        if k == 0:
            coefficients()
        w[k, rows] = rrow[k, N_, 0]

        @pl.when(lat_last)
        def _():
            w[k, rows] = folded(k, 0, w[k, rows - 1])

        def sides(v, ge, gw):
            ve = roll(jnp.where(lane == 0, ge, v), cols - 1)
            vw = roll(jnp.where(lane == cols - 1, gw, v), 1)
            return v, ve, vw

        prev = sides(rrow[k, S_, 0], rrow[k, SE_, 0], rrow[k, SW_, 0])
        gws, ges = [], []
        for h in range(halves):
            if h + 1 < halves:
                fe = roll(rcol[k, 0, h + 1], half)
                fw = roll(rcol[k, 1, h + 1], half)
            else:
                fe = roll(rrow[k, NE_, 0], half)
                fw = roll(rrow[k, NW_, 0], half + 1)
            ges.append(jnp.where(lane == half, fe, rcol[k, 0, h]))
            gws.append(jnp.where(lane == half, fw, rcol[k, 1, h]))
        cur = sides(w[k, 0], ges[0], roll(gws[0], cols - 1))
        acc0, acc1 = zero, zero
        for h in range(halves):
            ge_h, gw_h = ges[h], gws[h]

            def step(gl, carry):
                prev, cur, acc0, acc1, pw, pe, ge, gw = carry
                j0 = pl.multiple_of((h * steps + gl) * step_rows, 8)
                values = []
                for r in range(step_rows):
                    j = j0 + r
                    nxt = sides(w[k, j + 1], roll(ge, cols - 1 - r), roll(gw, cols - 2 - r))
                    c = [coef[q, pl.ds(j, 1), :] for q in range(8)]
                    out = (c[0] * cur[1] + c[1] * cur[2]) + (c[2] * nxt[0] + c[3] * prev[0])
                    out = out + ((c[4] * nxt[1] + c[5] * prev[2]) + (c[6] * nxt[2] + c[7] * prev[1]))
                    w[k + 1, j] = out
                    t = center[pl.ds(j, 1), :] * cur[0]
                    acc0 = acc0 + t * cur[0]
                    acc1 = acc1 + t * out
                    values.append(out)
                    prev, cur = cur, nxt
                if k + 1 < ITERS:
                    pw, pe = packed_step(pw, pe, values)
                ge, gw = roll(ge, cols - step_rows), roll(gw, cols - step_rows)
                return prev, cur, acc0, acc1, pw, pe, ge, gw
            prev, cur, acc0, acc1, pw, pe, _, _ = lax.fori_loop(
                0, steps, step, (prev, cur, acc0, acc1, zero, zero, ge_h, gw_h))
            if k + 1 < ITERS:
                colw[k + 1, h] = roll(pw, half)
                cole[k + 1, h] = roll(pe, half)
        if k + 1 < ITERS:
            rowtop[k + 1, 0] = w[k + 1, rows - 1]
            rowbot[k + 1, 0] = w[k + 1, 0]
        accs[:] = [acc0, acc1]
    add_sums()
    moments = zero
    for i, total in enumerate(sums):
        moments = jnp.where(lane == i, total, moments)

    def reduce(slot, value, recv, ss, rs, count, dev):
        red[slot] = value
        cps = [
            pltpu.make_async_remote_copy(
                src_ref=red.at[slot], dst_ref=recv.at[d], send_sem=ss.at[d],
                recv_sem=rs.at[d], device_id=dev(d), device_id_type=MESH)
            for d in range(1, count)
        ]
        for c in cps:
            c.start()
        for c in cps:
            c.wait_recv()
        for d in range(1, count):
            value = value + recv[d]
        return value, cps

    moments, c1 = reduce(0, moments, rred_lon, rl_ss, rl_rs, lon_count,
                         lambda d: (la, lax.rem(lo + d, lon_count)))
    moments, c2 = reduce(1, moments, rred_lat, rt_ss, rt_rs, lat_count,
                         lambda d: (lax.rem(la + d, lat_count), lo))

    m0, m1, m2, m3, m4, m5 = (
        jnp.broadcast_to(moments[:, i:i + 1], (members, cols)) for i in range(6))
    a0 = m1 / m0
    h1 = m2 - a0 * m1
    a1 = (m3 - 2.0 * a0 * m2 + a0 * a0 * m1) / h1
    b1 = h1 / m0
    p1 = -(a0 + a1)
    p0 = a0 * a1 - b1
    h2 = m4 + p1 * m3 + p0 * m2
    a2 = (m5 + p1 * m4 + p0 * m3) / h2 + p1
    b2 = h2 / h1
    t2 = p1 - a2
    t1 = p0 - a2 * p1 - b2
    t0 = b2 * a0 - a2 * p0
    q3 = 1.0 / (1.0 + t2 + t1 + t0)
    q2, q1, q0 = t2 * q3, t1 * q3, t0 * q3
    s2, s1, s0 = q3, q2 + q3, q1 + q2 + q3

    chunk = 4
    stores = []
    for c in range(chunk):
        size = groups // chunk

        def final(g, carry):
            for r in range(8):
                j = (c * size + g) * 8 + r
                v0, v1, v2, v3 = (w[i, j] for i in range(4))
                obuf[0, j] = s0 * v0 + s1 * v1 + s2 * v2
                obuf[1, j] = center[pl.ds(j, 1), :] * (q0 * v0 + q1 * v1 + q2 * v2 + q3 * v3)
            return carry
        lax.fori_loop(0, size, final, 0)
        rs = pl.ds(c * size * 8, size * 8)
        for o, dst in ((0, sol_out), (1, res_out)):
            for m in range(members):
                cp = pltpu.make_async_copy(
                    obuf.at[o, rs, m], dst.at[m, rs], store_sem.at[c, o, m])
                cp.start()
                stores.append(cp)
    for cps, folds in done:
        for cp in cps:
            cp.wait_send()

        @pl.when(lat_last)
        def _():
            for cp in folds:
                cp.wait_send()
    for cp in c1 + c2:
        cp.wait_send()
    for cp in stores:
        cp.wait()


def body(lat_count, lon_count, right_side, center, couplings, land_sea, fold_partner):
    members, rows, cols = right_side.shape
    f32 = jnp.float32
    halves = -(-rows // 120)
    hbm = pl.BlockSpec(memory_space=pl.ANY)
    dma = pltpu.SemaphoreType.DMA
    shape = jax.ShapeDtypeStruct(right_side.shape, f32)
    return pl.pallas_call(
        functools.partial(kernel, lat_count, lon_count),
        out_shape=(shape, shape),
        in_specs=[hbm] * 5,
        out_specs=(hbm, hbm),
        scratch_shapes=[
            pltpu.VMEM((ITERS + 1, rows + 1, members, cols), f32),
            pltpu.VMEM((2, rows, members, cols), f32),
            pltpu.VMEM((rows, cols), f32),
            pltpu.VMEM((4, rows, cols), f32),
            pltpu.VMEM((rows, cols), jnp.int32),
            pltpu.VMEM((lon_count, cols), jnp.int32),
            pltpu.VMEM((rows, cols), f32),
            pltpu.VMEM((8, rows, cols), f32),
            pltpu.VMEM((ITERS, 2, 8, cols), f32),
            pltpu.VMEM((ITERS, 1, 8, cols), f32),
            pltpu.VMEM((ITERS, halves + 1, 8, cols), f32),
            pltpu.VMEM((ITERS, halves + 1, 8, cols), f32),
            pltpu.VMEM((ITERS, 6, 2, 8, cols), f32),
            pltpu.VMEM((ITERS, 2, halves + 1, 8, cols), f32),
            pltpu.VMEM((ITERS, lon_count, 2, 8, cols), f32),
            pltpu.VMEM((2, 8, cols), f32),
            pltpu.VMEM((lon_count, 8, cols), f32),
            pltpu.VMEM((lat_count, 8, cols), f32),
            dma((4 + members,)),
            dma((4, 2, members)),
            dma((ITERS, 6)), dma((ITERS, 6)),
            dma((ITERS, 2)), dma((ITERS, 2)),
            dma((ITERS, lon_count)), dma((ITERS, lon_count)),
            dma((lon_count,)), dma((lon_count,)),
            dma((lat_count,)), dma((lat_count,)),
        ],
        compiler_params=pltpu.CompilerParams(
            collective_id=0, has_side_effects=True, vmem_limit_bytes=67043328),
    )(right_side, center, couplings, land_sea, fold_partner.reshape(lon_count, cols))


def solution(mesh):
    return jax.shard_map(
        functools.partial(body, mesh.shape["lat"], mesh.shape["lon"]),
        mesh=mesh,
        in_specs=(
            P(None, "lat", "lon"),
            P("lat", "lon"),
            P(None, "lat", "lon"),
            P("lat", "lon"),
            P(),
        ),
        out_specs=(P(None, "lat", "lon"), P(None, "lat", "lon")),
        check_vma=False,
    )
```

```python
import functools

import jax
import jax.numpy as jnp
from jax import lax
from jax.experimental import pallas as pl
from jax.experimental.pallas import tpu as pltpu
from jax.sharding import PartitionSpec as P

ITERS = 3
MESH = pl.DeviceIdType.MESH
S_, SE_, SW_, N_, NE_, NW_ = range(6)


def kernel(
    lat_count, lon_count,
    rhs, center_hbm, coup_hbm, land_hbm, partner_hbm, sol_out, res_out,
    w, obuf, center, coup, land, partner,
    dmask, coef, rowtop, rowbot, colw, cole, rrow, rcol, rfold, red, rred_lon, rred_lat,
    load_sem, store_sem, row_ss, row_rs, col_ss, col_rs, fold_ss, fold_rs,
    rl_ss, rl_rs, rt_ss, rt_rs,
):
    f32 = jnp.float32
    members, rows, cols = rhs.shape
    groups = rows // 8
    halves = -(-rows // 120)
    half = rows // halves
    step_rows = 24 if half % 24 == 0 else 8
    steps = half // step_rows
    la, lo = lax.axis_index("lat"), lax.axis_index("lon")
    lat_first, lat_last = la == 0, la == lat_count - 1
    north, south = lax.rem(la + 1, lat_count), lax.rem(la + lat_count - 1, lat_count)
    east, west = lax.rem(lo + 1, lon_count), lax.rem(lo + lon_count - 1, lon_count)
    lane = lax.broadcasted_iota(jnp.int32, (members, cols), 1)
    sub = lax.broadcasted_iota(jnp.int32, (8, cols), 0)

    loads = [
        pltpu.make_async_copy(center_hbm, center, load_sem.at[0]),
        pltpu.make_async_copy(coup_hbm, coup, load_sem.at[1]),
        pltpu.make_async_copy(land_hbm, land, load_sem.at[2]),
        pltpu.make_async_copy(partner_hbm, partner, load_sem.at[3]),
    ]
    for m in range(members):
        loads.append(pltpu.make_async_copy(
            rhs.at[m], w.at[0, pl.ds(0, rows), m], load_sem.at[4 + m]))
    for c in loads:
        c.start()

    barrier = pltpu.get_barrier_semaphore()
    partners = [(la, lax.rem(lo + d, lon_count)) for d in range(1, lon_count)]
    partners += [(lax.rem(la + d, lat_count), lo) for d in range(1, lat_count)]
    partners += [(north, east), (north, west), (south, east), (south, west)]
    for p in partners:
        pl.semaphore_signal(barrier, inc=1, device_id=p, device_id_type=MESH)

    for c in loads:
        c.wait()

    def roll(x, shift, axis=1):
        return pltpu.roll(x, shift, axis)

    def packed_step(pw, pe, values):
        pw, pe = roll(pw, cols - step_rows), roll(pe, cols - step_rows)
        for r, v in enumerate(values):
            at = cols - step_rows + r
            pw = jnp.where(lane == at, roll(v, at), pw)
            pe = jnp.where(lane == at, roll(v, (at + 1) % cols), pe)
        return pw, pe

    for h in range(halves):
        def prep(gl, carry):
            pw, pe = carry
            j0 = pl.multiple_of((h * steps + gl) * step_rows, 8)
            rs = pl.ds(j0, step_rows)
            dmask[rs, :] = land[rs, :].astype(f32) / center[rs, :]
            values = []
            for r in range(step_rows):
                v = w[0, j0 + r] * dmask[pl.ds(j0 + r, 1), :]
                w[0, j0 + r] = v
                values.append(v)
            return packed_step(pw, pe, values)
        zero = jnp.zeros((members, cols), f32)
        pw, pe = lax.fori_loop(0, steps, prep, (zero, zero))
        colw[0, h] = roll(pw, half)
        cole[0, h] = roll(pe, half)
    cw = jnp.zeros((8, cols), f32)
    ce = jnp.zeros((8, cols), f32)
    for g in range(groups):
        rs = pl.ds(g * 8, 8)
        ce = jnp.where(lane == g, roll(coup[0, rs, :], g + 1), ce)
        ce = jnp.where(lane == groups + g, roll(coup[2, rs, :], groups + g + 1), ce)
        cw = jnp.where(lane == g, roll(coup[3, rs, :], g) if g else coup[3, rs, :], cw)
    colw[0, halves] = cw
    cole[0, halves] = ce
    rowtop[0, 0] = w[0, rows - 1]
    rowbot[0, 0] = w[0, 0]
    top = [coup[c, pl.ds(rows - 1, 1), :] for c in range(4)]
    packed = jnp.zeros((8, cols), f32)
    for c in (1, 2, 3):
        packed = jnp.where(sub == c, top[c], packed)
    rowtop[0, 1] = packed

    pl.semaphore_wait(barrier, len(partners))

    def exchange(k, between):
        tops = 2 if k == 0 else 1
        depth = halves + 1 if k == 0 else halves
        cps = []

        def rcopy(src, slot, n, dev):
            cps.append(pltpu.make_async_remote_copy(
                src_ref=src.at[k, pl.ds(0, n)], dst_ref=rrow.at[k, slot, pl.ds(0, n)],
                send_sem=row_ss.at[k, slot], recv_sem=row_rs.at[k, slot],
                device_id=dev, device_id_type=MESH))
        rcopy(rowtop, SW_, tops, (north, east))
        rcopy(rowtop, SE_, tops, (north, west))
        rcopy(rowbot, NW_, 1, (south, east))
        rcopy(rowbot, NE_, 1, (south, west))
        rcopy(rowtop, S_, tops, (north, lo))
        rcopy(rowbot, N_, 1, (south, lo))
        for src, side, dev in ((colw, 0, west), (cole, 1, east)):
            cps.append(pltpu.make_async_remote_copy(
                src_ref=src.at[k, pl.ds(0, depth)], dst_ref=rcol.at[k, side, pl.ds(0, depth)],
                send_sem=col_ss.at[k, side], recv_sem=col_rs.at[k, side],
                device_id=(la, dev), device_id_type=MESH))
        folds = []
        for d in range(1, lon_count):
            folds.append(pltpu.make_async_remote_copy(
                src_ref=rowtop.at[k, pl.ds(0, tops)], dst_ref=rfold.at[k, d, pl.ds(0, tops)],
                send_sem=fold_ss.at[k, d], recv_sem=fold_rs.at[k, d],
                device_id=(la, lax.rem(lo + d, lon_count)), device_id_type=MESH))

        @pl.when(lat_last)
        def _():
            for c in folds:
                c.start()
        for c in cps:
            c.start()
        between()
        for c in cps:
            c.wait_recv()

        @pl.when(lat_last)
        def _():
            for c in folds:
                c.wait_recv()
        return cps, folds

    def folded(k, slot, own):
        mine = partner[pl.ds(lo, 1), :]
        out = jnp.zeros((8, cols), f32)
        for d in range(lon_count):
            data = own if d == 0 else rfold[k, d, slot]
            first = lax.rem(lo + lon_count - d, lon_count) * cols
            at = jnp.broadcast_to(mine - first, (8, cols))
            inside = jnp.logical_and(at >= 0, at < cols)
            at = jnp.clip(at, 0, cols - 1)
            got = jnp.take_along_axis(data, at, axis=1, mode="promise_in_bounds")
            out = jnp.where(inside, got, out)
        return out

    done = []
    lane8 = lax.broadcasted_iota(jnp.int32, (8, cols), 1)

    def coefficients():
        smsg, semsg, swmsg = rrow[0, S_, 1], rrow[0, SE_, 1], rrow[0, SW_, 1]
        keep = jnp.where(lat_first, 0.0, 1.0).astype(f32)
        under_n = roll(smsg, 7, 0) * keep
        under_ne = roll(roll(jnp.where(lane8 == cols - 1, swmsg, smsg), 1), 6, 0) * keep
        under_nw = roll(roll(jnp.where(lane8 == 0, semsg, smsg), cols - 1), 5, 0) * keep
        from_east, from_west = rcol[0, 0, halves], rcol[0, 1, halves]

        @pl.when(lat_last)
        def _():
            got = folded(0, 1, rowtop[0, 1])
            last = rows - 1
            coup[1, pl.ds(last, 1), :] = 0.5 * (coup[1, pl.ds(last, 1), :] + got[1:2, :])
            coup[2, pl.ds(last, 1), :] = jnp.zeros((1, cols), f32)
            coup[3, pl.ds(last, 1), :] = jnp.zeros((1, cols), f32)

        def step(g, carry):
            pn, pne, pnw = carry
            rs = pl.ds(pl.multiple_of(g * 8, 8), 8)
            d = dmask[rs, :]
            e, n, ne, nw = (coup[c, rs, :] for c in range(4))
            gw = roll(from_west, lax.rem(2 * cols - 1 - g, cols))
            gne = roll(from_west, lax.rem(2 * cols - 1 - groups - g, cols))
            gnw = roll(from_east, lax.rem(cols - g, cols))
            coef[0, rs, :] = e * d
            coef[1, rs, :] = roll(jnp.where(lane8 == cols - 1, gw, e), 1) * d
            coef[2, rs, :] = n * d
            ns = roll(n, 1, 0)
            coef[3, rs, :] = jnp.where(sub == 0, pn, ns) * d
            coef[4, rs, :] = ne * d
            nes = roll(roll(jnp.where(lane8 == cols - 1, gne, ne), 1), 1, 0)
            coef[5, rs, :] = jnp.where(sub == 0, pne, nes) * d
            coef[6, rs, :] = nw * d
            nws = roll(roll(jnp.where(lane8 == 0, gnw, nw), cols - 1), 1, 0)
            coef[7, rs, :] = jnp.where(sub == 0, pnw, nws) * d
            return ns, nes, nws
        lax.fori_loop(0, groups, step, (under_n, under_ne, under_nw), unroll=12)

    zero = jnp.zeros((members, cols), f32)
    sums = []

    def add_sums():
        for acc in accs:
            sums.append(jnp.sum(acc, axis=1, keepdims=True))

    accs = []
    for k in range(ITERS):
        done.append(exchange(k, add_sums))
        if k == 0:
            coefficients()
        w[k, rows] = rrow[k, N_, 0]

        @pl.when(lat_last)
        def _():
            w[k, rows] = folded(k, 0, w[k, rows - 1])

        def sides(v, ge, gw):
            ve = roll(jnp.where(lane == 0, ge, v), cols - 1)
            vw = roll(jnp.where(lane == cols - 1, gw, v), 1)
            return v, ve, vw

        prev = sides(rrow[k, S_, 0], rrow[k, SE_, 0], rrow[k, SW_, 0])
        gws, ges = [], []
        for h in range(halves):
            if h + 1 < halves:
                fe = roll(rcol[k, 0, h + 1], half)
                fw = roll(rcol[k, 1, h + 1], half)
            else:
                fe = roll(rrow[k, NE_, 0], half)
                fw = roll(rrow[k, NW_, 0], half + 1)
            ges.append(jnp.where(lane == half, fe, rcol[k, 0, h]))
            gws.append(jnp.where(lane == half, fw, rcol[k, 1, h]))
        cur = sides(w[k, 0], ges[0], roll(gws[0], cols - 1))
        acc0, acc1 = zero, zero
        for h in range(halves):
            ge_h, gw_h = ges[h], gws[h]

            def step(gl, carry):
                prev, cur, acc0, acc1, pw, pe, ge, gw = carry
                j0 = pl.multiple_of((h * steps + gl) * step_rows, 8)
                values = []
                for r in range(step_rows):
                    j = j0 + r
                    nxt = sides(w[k, j + 1], roll(ge, cols - 1 - r), roll(gw, cols - 2 - r))
                    c = [coef[q, pl.ds(j, 1), :] for q in range(8)]
                    out = (c[0] * cur[1] + c[1] * cur[2]) + (c[2] * nxt[0] + c[3] * prev[0])
                    out = out + ((c[4] * nxt[1] + c[5] * prev[2]) + (c[6] * nxt[2] + c[7] * prev[1]))
                    w[k + 1, j] = out
                    t = center[pl.ds(j, 1), :] * cur[0]
                    acc0 = acc0 + t * cur[0]
                    acc1 = acc1 + t * out
                    values.append(out)
                    prev, cur = cur, nxt
                if k + 1 < ITERS:
                    pw, pe = packed_step(pw, pe, values)
                ge, gw = roll(ge, cols - step_rows), roll(gw, cols - step_rows)
                return prev, cur, acc0, acc1, pw, pe, ge, gw
            prev, cur, acc0, acc1, pw, pe, _, _ = lax.fori_loop(
                0, steps, step, (prev, cur, acc0, acc1, zero, zero, ge_h, gw_h))
            if k + 1 < ITERS:
                colw[k + 1, h] = roll(pw, half)
                cole[k + 1, h] = roll(pe, half)
        if k + 1 < ITERS:
            rowtop[k + 1, 0] = w[k + 1, rows - 1]
            rowbot[k + 1, 0] = w[k + 1, 0]
        accs[:] = [acc0, acc1]
    add_sums()
    moments = zero
    for i, total in enumerate(sums):
        moments = jnp.where(lane == i, total, moments)

    def reduce(slot, value, recv, ss, rs, count, dev):
        red[slot] = value
        cps = [
            pltpu.make_async_remote_copy(
                src_ref=red.at[slot], dst_ref=recv.at[d], send_sem=ss.at[d],
                recv_sem=rs.at[d], device_id=dev(d), device_id_type=MESH)
            for d in range(1, count)
        ]
        for c in cps:
            c.start()
        for c in cps:
            c.wait_recv()
        for d in range(1, count):
            value = value + recv[d]
        return value, cps

    moments, c1 = reduce(0, moments, rred_lon, rl_ss, rl_rs, lon_count,
                         lambda d: (la, lax.rem(lo + d, lon_count)))
    moments, c2 = reduce(1, moments, rred_lat, rt_ss, rt_rs, lat_count,
                         lambda d: (lax.rem(la + d, lat_count), lo))

    m0, m1, m2, m3, m4, m5 = (
        jnp.broadcast_to(moments[:, i:i + 1], (members, cols)) for i in range(6))
    a0 = m1 / m0
    h1 = m2 - a0 * m1
    a1 = (m3 - 2.0 * a0 * m2 + a0 * a0 * m1) / h1
    b1 = h1 / m0
    p1 = -(a0 + a1)
    p0 = a0 * a1 - b1
    h2 = m4 + p1 * m3 + p0 * m2
    a2 = (m5 + p1 * m4 + p0 * m3) / h2 + p1
    b2 = h2 / h1
    t2 = p1 - a2
    t1 = p0 - a2 * p1 - b2
    t0 = b2 * a0 - a2 * p0
    q3 = 1.0 / (1.0 + t2 + t1 + t0)
    q2, q1, q0 = t2 * q3, t1 * q3, t0 * q3
    s2, s1, s0 = q3, q2 + q3, q1 + q2 + q3

    chunk = 4
    stores = []
    for c in range(chunk):
        size = groups // chunk

        def final(g, carry):
            for r in range(8):
                j = (c * size + g) * 8 + r
                v0, v1, v2, v3 = (w[i, j] for i in range(4))
                obuf[0, j] = s0 * v0 + s1 * v1 + s2 * v2
                obuf[1, j] = center[pl.ds(j, 1), :] * (q0 * v0 + q1 * v1 + q2 * v2 + q3 * v3)
            return carry
        lax.fori_loop(0, size, final, 0)
        rs = pl.ds(c * size * 8, size * 8)
        for o, dst in ((0, sol_out), (1, res_out)):
            for m in range(members):
                cp = pltpu.make_async_copy(
                    obuf.at[o, rs, m], dst.at[m, rs], store_sem.at[c, o, m])
                cp.start()
                stores.append(cp)
    for cps, folds in done:
        for cp in cps:
            cp.wait_send()

        @pl.when(lat_last)
        def _():
            for cp in folds:
                cp.wait_send()
    for cp in c1 + c2:
        cp.wait_send()
    for cp in stores:
        cp.wait()


def body(lat_count, lon_count, right_side, center, couplings, land_sea, fold_partner):
    members, rows, cols = right_side.shape
    f32 = jnp.float32
    halves = -(-rows // 120)
    hbm = pl.BlockSpec(memory_space=pl.ANY)
    dma = pltpu.SemaphoreType.DMA
    shape = jax.ShapeDtypeStruct(right_side.shape, f32)
    return pl.pallas_call(
        functools.partial(kernel, lat_count, lon_count),
        out_shape=(shape, shape),
        in_specs=[hbm] * 5,
        out_specs=(hbm, hbm),
        scratch_shapes=[
            pltpu.VMEM((ITERS + 1, rows + 1, members, cols), f32),
            pltpu.VMEM((2, rows, members, cols), f32),
            pltpu.VMEM((rows, cols), f32),
            pltpu.VMEM((4, rows, cols), f32),
            pltpu.VMEM((rows, cols), jnp.int32),
            pltpu.VMEM((lon_count, cols), jnp.int32),
            pltpu.VMEM((rows, cols), f32),
            pltpu.VMEM((8, rows, cols), f32),
            pltpu.VMEM((ITERS, 2, 8, cols), f32),
            pltpu.VMEM((ITERS, 1, 8, cols), f32),
            pltpu.VMEM((ITERS, halves + 1, 8, cols), f32),
            pltpu.VMEM((ITERS, halves + 1, 8, cols), f32),
            pltpu.VMEM((ITERS, 6, 2, 8, cols), f32),
            pltpu.VMEM((ITERS, 2, halves + 1, 8, cols), f32),
            pltpu.VMEM((ITERS, lon_count, 2, 8, cols), f32),
            pltpu.VMEM((2, 8, cols), f32),
            pltpu.VMEM((lon_count, 8, cols), f32),
            pltpu.VMEM((lat_count, 8, cols), f32),
            dma((4 + members,)),
            dma((4, 2, members)),
            dma((ITERS, 6)), dma((ITERS, 6)),
            dma((ITERS, 2)), dma((ITERS, 2)),
            dma((ITERS, lon_count)), dma((ITERS, lon_count)),
            dma((lon_count,)), dma((lon_count,)),
            dma((lat_count,)), dma((lat_count,)),
        ],
        compiler_params=pltpu.CompilerParams(
            collective_id=0, has_side_effects=True, vmem_limit_bytes=67043328),
    )(right_side, center, couplings, land_sea, fold_partner.reshape(lon_count, cols))


def solution(mesh):
    return jax.shard_map(
        functools.partial(body, mesh.shape["lat"], mesh.shape["lon"]),
        mesh=mesh,
        in_specs=(
            P(None, "lat", "lon"),
            P("lat", "lon"),
            P(None, "lat", "lon"),
            P("lat", "lon"),
            P(),
        ),
        out_specs=(P(None, "lat", "lon"), P(None, "lat", "lon")),
        check_vma=False,
    )
```
